32 devices in a mesh: shard: 8 (over z, x), rep: 4 (over y, core).
Axes of the slice: x: 2, y: 2, z: 4, core: 2. Of those that a mesh axis runs over, the one named last changes fastest.
Arguments:
- activations: bfloat16 [4, 2048, 2048], P(None, ('shard', 'rep')), may hold values from -6 to 6
- value_grad: bfloat16 [4, 2048, 512], P(None, ('shard', 'rep')), may hold values from -6 to 6
- norm_gain: bfloat16 [2048], P('shard'), may hold values from 0.25 to 4.5
- value_weight: bfloat16 [2048, 512], P('shard'), may hold values from -0.125 to 0.125
Outputs:
- input_grad: bfloat16 [4, 2048, 2048], P(None, ('shard', 'rep'))
- weight_update: float32 [2048, 512], P('shard')
The draws below stay inside these ranges and needn't reach their ends.
All inputs are finite; a program needn't handle non-finite values.
Results may differ from the reference program's by a relative error of at most 0.0029.
Values may be sent and summed in bfloat16 or wider, within the bound.
No kernel may reach another device: no remote copies, remote signals or barrier semaphores. Data moves between devices by JAX's collectives and lax.ppermute only.
A program may use at most 64 MiB of HBM per device.

```python
import jax
import jax.numpy as jnp
from jax import lax

D = 2048
VW = 512
MB = 4
TOKENS = 2048


def draw_norm_gain(key, part):
    where = jnp.arange(D, dtype=jnp.float32) / D
    noise = jax.random.uniform(key, (D,), jnp.float32, -0.4, 0.4)
    base = 0.6 + 1.2 * where
    return (base * jnp.exp(noise)).astype(jnp.bfloat16)


def spiked(values, key, source, target, shards_of, factor):
    owner, partner = [(jnp.arange(values.shape[position]) // (values.shape[position] // shards_of)).reshape([-1 if axis == position else 1 for axis in range(values.ndim)]) for position in (source, target)]
    chosen = jax.random.permutation(key, shards_of)[partner]
    strong = (owner == chosen) | (owner == (partner + shards_of // 2) % shards_of)
    return jnp.where(strong, factor * values, values)


def level_of(stream_key, extent, cuts, low, largest):
    def one(axis_at, parts):
        steps = jax.random.uniform(jax.random.fold_in(jax.random.fold_in(stream_key, 6), axis_at), (parts,), jnp.float32, low / len(cuts), largest / len(cuts))
        return jnp.repeat(jnp.exp(steps), extent[axis_at] // parts).reshape((-1,) + (1,) * (len(extent) - axis_at - 1))

    factor_of = one(*cuts[0])
    for cut in cuts[1:]:
        factor_of = factor_of * one(*cut)
    return factor_of


def bell_draw(own_key, shape, spread, bound, shards=(), kind=jnp.bfloat16):
    loudness = level_of(own_key, shape, shards, -0.22, 0.18) if shards else 1.0
    drawn = jax.random.normal(own_key, shape, jnp.float32) * spread * loudness
    return jnp.minimum(jnp.maximum(drawn, -bound), bound).astype(kind)


def bell_draw_with(key, dims, width, limit, pieces, heavy, kind=jnp.bfloat16):
    entries = width * jax.random.normal(key, dims, jnp.float32)
    if pieces:
        entries = entries * level_of(key, dims, pieces, -0.22, 0.18)
    return jnp.clip(spiked(entries, jax.random.fold_in(key, 3), *heavy), -limit, limit).astype(kind)


def setup_inputs(seed: int = 0) -> dict:
    splits = jax.random.split(jax.random.key(seed), 5)
    return {
        "activations": bell_draw_with(splits[0], (MB, TOKENS, D), 1.0, 6.0, ((1, 32),), (1, 2, 32, 2.75)),
        "value_grad": bell_draw(splits[1], (MB, TOKENS, VW), 1.0, 6.0, ((1, 32),)),
        "norm_gain": draw_norm_gain(jax.random.fold_in(splits[4], 71), 0),
        "value_weight": bell_draw(splits[3], (D, VW), D ** -0.5, 0.125, ((0, 8),)),
    }


def reference(activations, value_grad, norm_gain, value_weight):
    gain = norm_gain.astype(jnp.float32)

    def one_batch(total, inputs):
        block, cotangent = inputs
        values = block.astype(jnp.float32)
        rstd = lax.rsqrt(lax.optimization_barrier(jnp.mean(values * values, axis=-1, keepdims=True)) + 1e-05)
        normed = (values * rstd * gain).astype(jnp.bfloat16)
        total = total + lax.dot_general(normed, cotangent, (((0,), (0,)), ((), ())), preferred_element_type=jnp.float32)
        normed_grad = jnp.dot(cotangent, value_weight.T, preferred_element_type=jnp.float32)
        scaled = normed_grad * gain
        inner = lax.optimization_barrier(jnp.mean(scaled * values, axis=-1, keepdims=True))
        result = (rstd * scaled - values * rstd * rstd * rstd * inner).astype(jnp.bfloat16)
        return (total, result)
    start = jnp.zeros((D, VW), jnp.float32)
    grad, input_grad = lax.scan(one_batch, start, (activations, value_grad))
    squares = jnp.sum(grad * grad)
    factor = 1.0 / jnp.maximum(1.0, jnp.sqrt(squares / (D * VW)))
    return (input_grad, grad * factor)
```

```python
import functools

import jax
import jax.numpy as jnp
from jax import lax
from jax.experimental import pallas as pl
from jax.experimental.pallas import tpu as pltpu
from jax.sharding import PartitionSpec as P


F32, BF16 = jnp.float32, jnp.bfloat16
LANES = 128
VMEM = pl.BlockSpec(memory_space=pltpu.VMEM)


def ab(m, n, ca, cb):
    return lax.dot_general(m, n, (((ca,), (cb,)), ((), ())), preferred_element_type=F32)


def place(reps):
    rep = lax.axis_index("rep")
    return lax.axis_index("shard"), rep // 2, rep % 2


def row_rstd(values):
    return lax.rsqrt(jnp.mean(values * values, axis=-1, keepdims=True) + 1e-05)


def grad_kernel(reps, zs, rows, a0, a1, v0, v1, keep, send_x, send_y, send_d, high, low, left):
    shard, y, core = place(reps)
    x = shard % 2
    tokens, half, wide = a0.shape[0], rows // 2, keep.shape[1]
    for part, (acts, cot) in enumerate(((a0, v0), (a1, v1))):
        scaled = cot[...].astype(F32) * row_rstd(acts[...].astype(F32))
        top = scaled.astype(BF16)
        high[pl.ds(part * tokens, tokens), :] = top
        low[pl.ds(part * tokens, tokens), :] = (scaled - top.astype(F32)).astype(BF16)
    for dx in range(2):
        for z in range(zs):
            at = pl.multiple_of((2 * z + (x ^ dx)) * rows + core * half, LANES)
            for part, acts in enumerate((a0, a1)):
                left[pl.ds(part * tokens, tokens), pl.ds((dx * zs + z) * half, half)] = acts[:, pl.ds(at, half)]
    for dx, dy, out in ((1, 1, send_d), (0, 1, send_y), (1, 0, send_x), (0, 0, keep)):
        cols = pl.ds(pl.multiple_of((y ^ dy) * wide, LANES), wide)
        mine = left[:, pl.ds(dx * zs * half, zs * half)]
        out[...] = (ab(mine, high[:, cols], 0, 0) + ab(mine, low[:, cols], 0, 0)).astype(out.dtype)


def plane_kernel(reps, zs, keep, got_x, got_y, got_d, mine, *sends):
    shard, _, _ = place(reps)
    z, half = shard // 2, mine.shape[0]
    for k, out in ((k, sends[k - 1] if k else mine) for k in (*range(1, zs), 0)):
        at = pl.ds(pl.multiple_of((z ^ k) * half, LANES), half)
        total = (keep[at, :] + got_x[at, :].astype(F32)) + (got_y[at, :].astype(F32) + got_d[at, :].astype(F32))
        out[...] = total.astype(out.dtype)


def line_kernel(reps, mine, *refs):
    *got, gain, piece, squares = refs
    _, _, core = place(reps)
    half = mine.shape[0]
    total = mine[...]
    for other in got:
        total = total + other[...].astype(F32)
    total = total * gain[pl.ds(pl.multiple_of(core * half, LANES), half), :].astype(F32)
    piece[...] = total
    squares[...] = jnp.full(squares.shape, jnp.sum(total * total), F32)


def scale_kernel(reps, count, own, got_y, got_c, got_cy, s0, s1, s2, s3, out):
    _, y, core = place(reps)
    half, wide = own.shape
    squares = ((s0[...] + s1[...]) + (s2[...] + s3[...]))[:1, :1]
    factor = 1.0 / jnp.maximum(1.0, jnp.sqrt(squares / count))
    for dc, dy, piece in ((0, 0, own), (0, 1, got_y), (1, 0, got_c), (1, 1, got_cy)):
        at = pl.ds(pl.multiple_of((core ^ dc) * half, LANES), half)
        out[at, pl.ds(pl.multiple_of((y ^ dy) * wide, LANES), wide)] = piece[...] * factor


def input_kernel(reps, rows, order, acts, cot, own, other, out, scaled):
    shard, _, core = place(reps)
    shards, half = own.shape[0], rows // 2
    inner = jnp.zeros((acts.shape[0], LANES), F32)
    for ref, c in ((own, core), (other, 1 - core)):
        for j in range(0, shards, 2):
            pair = jnp.concatenate([ref[j, :half, :], ref[j + 1, :half, :]], axis=0)
            product = ab(cot[...], pair, 1, 1)
            for k in range(2):
                col = pl.ds(pl.multiple_of((shard ^ order[j + k]) * rows + c * half, LANES), half)
                gain = ref[j + k, pl.ds(half, 8), pl.ds(pl.multiple_of(c * half, LANES), half)][:1].astype(F32)
                h = product[:, k * half : (k + 1) * half] * gain
                scaled[:, col] = h
                inner = inner + h * acts[:, col].astype(F32)
    width = acts.shape[1]
    values = acts[...].astype(F32)
    rstd = row_rstd(values)
    mean = jnp.sum(inner, axis=-1, keepdims=True) * (1.0 / width)
    out[...] = (rstd * scaled[...] - values * (rstd * rstd * rstd * mean)).astype(out.dtype)


def call(kernel, shapes, *args, scratch=()):
    return pl.pallas_call(
        kernel,
        out_shape=shapes,
        in_specs=[VMEM] * len(args),
        out_specs=jax.tree.map(lambda _: VMEM, shapes),
        scratch_shapes=scratch,
        name=(kernel.func if isinstance(kernel, functools.partial) else kernel).__name__,
        compiler_params=pltpu.CompilerParams(vmem_limit_bytes=48 * 2**20),
    )(*args)


def fast(shards, reps, activations, value_grad, norm_gain, value_weight):
    batches, tokens, width = activations.shape
    rows, columns = value_weight.shape
    zs, half, wide = shards // 2, rows // 2, columns // 2
    tokens *= batches
    acts, cot = activations.reshape(tokens, width), value_grad.reshape(tokens, columns)

    def swap(value, over_shard, over_rep):
        pairs = [
            (s * reps + r, (s ^ over_shard) * reps + (r ^ over_rep)) for s in range(shards) for r in range(reps)
        ]
        return lax.ppermute(value, ("shard", "rep"), pairs)

    def like(*shape, kind=F32):
        return jax.ShapeDtypeStruct(shape, kind)

    acts_other, cot_other = swap(acts, 0, 1), swap(cot, 0, 1)

    core = lax.axis_index("rep") % 2
    gain_row = jnp.pad(norm_gain[None, :], ((0, 15), (0, columns - rows)))
    held = jnp.concatenate([lax.dynamic_slice_in_dim(value_weight, core * half, half, 0), gain_row], axis=0)[None]
    order = [0]
    for bit in (2, 4, 1):
        held = jnp.concatenate([held, swap(held, bit, 0)], axis=0)
        order += [j ^ bit for j in order]
    held_other = swap(held, 0, 1)

    keep, send_x, send_y, send_d = call(
        functools.partial(grad_kernel, reps, zs, rows),
        (like(zs * half, wide),) + (like(zs * half, wide, kind=BF16),) * 3,
        acts, acts_other, cot, cot_other,
        scratch=[
            pltpu.VMEM((2 * tokens, columns), BF16),
            pltpu.VMEM((2 * tokens, columns), BF16),
            pltpu.VMEM((2 * tokens, 2 * zs * half), BF16),
        ],
    )
    got_d, got_y, got_x = swap(send_d, 1, 2), swap(send_y, 0, 2), swap(send_x, 1, 0)
    mine, *sends = call(
        functools.partial(plane_kernel, reps, zs),
        (like(half, wide),) + (like(half, wide, kind=BF16),) * (zs - 1),
        keep, got_x, got_y, got_d,
    )
    got = [swap(sends[k - 1], 2 * k, 0) for k in range(1, zs)]
    own, squares = call(
        functools.partial(line_kernel, reps),
        (like(half, wide), like(8, LANES)),
        mine, *got, norm_gain[:, None],
    )
    got_y = swap(own, 0, 2)
    got_c = swap(own, 0, 1)
    got_cy = swap(got_y, 0, 1)
    squares = squares + swap(squares, 0, 1)
    squares = (squares + swap(squares, 1, 0)) + (swap(squares, 0, 2) + swap(squares, 1, 2))
    parts = [squares] + [swap(squares, 2 * k, 0) for k in range(1, zs)]
    update = call(
        functools.partial(scale_kernel, reps, float(width * columns)),
        like(rows, columns),
        own, got_y, got_c, got_cy, *parts,
    )
    result = call(
        functools.partial(input_kernel, reps, rows, order),
        like(tokens, width, kind=BF16),
        acts, cot, held, held_other,
        scratch=[pltpu.VMEM((tokens, width), F32)],
    )
    return result.reshape(activations.shape), update


def plain(shards, reps, activations, value_grad, norm_gain, value_weight):
    gain_all, weight_all = (
        lax.all_gather(norm_gain, "shard", axis=0, tiled=True),
        lax.all_gather(value_weight, "shard", axis=0, tiled=True),
    )
    gain = gain_all.astype(F32)
    width = activations.shape[2]
    columns = value_grad.shape[2]

    def one_batch(total, inputs):
        block, cotangent = inputs
        values = block.astype(F32)
        rstd = row_rstd(values)
        normed = (values * rstd * gain).astype(BF16)
        total = total + ab(normed, cotangent, 0, 0)
        scaled = jnp.dot(cotangent, weight_all.T, preferred_element_type=F32) * gain
        inner = jnp.mean(scaled * values, axis=-1, keepdims=True)
        result = (rstd * scaled - values * rstd * rstd * rstd * inner).astype(BF16)
        return (total, result)

    start = jnp.zeros((width, columns), F32)
    grad_full, input_grad = lax.scan(one_batch, start, (activations, value_grad))
    partial_rows = lax.psum_scatter(grad_full, "shard", scatter_dimension=0, tiled=True)
    summed = lax.psum(partial_rows, "rep")
    squares = lax.psum(jnp.sum(summed * summed), "shard")
    factor = 1.0 / jnp.maximum(1.0, jnp.sqrt(squares / (width * columns)))
    return (input_grad, summed * factor)


def solution(mesh):
    shards, reps = mesh.shape["shard"], mesh.shape["rep"]

    def on_device(activations, value_grad, norm_gain, value_weight):
        rows, columns = value_weight.shape
        fits = (shards, reps) == (8, 4) and rows % 256 == 0 and columns % 256 == 0 and rows <= columns
        return (fast if fits else plain)(shards, reps, activations, value_grad, norm_gain, value_weight)

    in_specs = (
        P(None, ("shard", "rep"), None),
        P(None, ("shard", "rep"), None),
        P("shard"),
        P("shard", None),
    )
    out_specs = (P(None, ("shard", "rep"), None), P("shard", None))
    return jax.shard_map(on_device, mesh=mesh, in_specs=in_specs, out_specs=out_specs, check_vma=False)
```

```python
import functools

import jax
import jax.numpy as jnp
from jax import lax
from jax.experimental import pallas as pl
from jax.experimental.pallas import tpu as pltpu
from jax.sharding import PartitionSpec as P


F32, BF16 = jnp.float32, jnp.bfloat16
LANES = 128
VMEM = pl.BlockSpec(memory_space=pltpu.VMEM)


def ab(m, n, ca, cb):
    return lax.dot_general(m, n, (((ca,), (cb,)), ((), ())), preferred_element_type=F32)


def place():
    rep = lax.axis_index("rep")
    return lax.axis_index("shard"), rep // 2, rep % 2


def row_rstd(values):
    return lax.rsqrt(jnp.mean(values * values, axis=-1, keepdims=True) + 1e-05)


def split_tokens(acts, cot, high, low):
    scaled = cot[...].astype(F32) * row_rstd(acts[...].astype(F32))
    top = scaled.astype(BF16)
    high[...] = top
    low[...] = (scaled - top.astype(F32)).astype(BF16)


def gather_columns(zs, rows, place, acts, left):
    shard, _, core = place
    half = rows // 2
    for dx in range(2):
        for z in range(zs):
            at = pl.multiple_of((2 * z + (shard % 2 ^ dx)) * rows + core * half, LANES)
            left[:, pl.ds((dx * zs + z) * half, half)] = acts[:, pl.ds(at, half)]


def piece(y, dx, dy, left, high, low):
    wide, height = high.shape[1] // 2, left.shape[1] // 2
    cols = pl.ds(pl.multiple_of((y ^ dy) * wide, LANES), wide)
    mine = left[:, pl.ds(dx * height, height)]
    return ab(mine, high[:, cols], 0, 0) + ab(mine, low[:, cols], 0, 0)


PIECES = ((1, 1), (0, 1), (1, 0), (0, 0))


def own_kernel(zs, rows, acts_hbm, cot_hbm, part, acts, cot, high, low, left, sems):
    copies = [
        pltpu.make_async_copy(source, target, sems.at[n])
        for n, (source, target) in enumerate(((acts_hbm, acts), (cot_hbm, cot)))
    ]
    for copy in copies:
        copy.start()
    for copy in copies:
        copy.wait()
    _, y, _ = where = place()
    split_tokens(acts, cot, high, low)
    gather_columns(zs, rows, where, acts, left)
    for n, (dx, dy) in enumerate(PIECES):
        part[n] = piece(y, dx, dy, left, high, low)


def grad_kernel(zs, rows, acts, cot, part, send_d, send_y, send_x, keep, high, low, left):
    _, y, _ = where = place()
    split_tokens(acts, cot, high, low)
    gather_columns(zs, rows, where, acts, left)
    for n, ((dx, dy), out) in enumerate(zip(PIECES, (send_d, send_y, send_x, keep))):
        out[...] = (part[n] + piece(y, dx, dy, left, high, low)).astype(out.dtype)


def plane_kernel(zs, keep, got_x, got_y, got_d, mine, *sends):
    shard, _, _ = place()
    z, half = shard // 2, mine.shape[0]
    for k, out in ((k, sends[k - 1] if k else mine) for k in (*range(1, zs), 0)):
        at = pl.ds(pl.multiple_of((z ^ k) * half, LANES), half)
        total = (keep[at, :] + got_x[at, :].astype(F32)) + (got_y[at, :].astype(F32) + got_d[at, :].astype(F32))
        out[...] = total.astype(out.dtype)


def line_kernel(mine, *refs):
    *got, gain, piece, squares = refs
    _, _, core = place()
    half = mine.shape[0]
    total = mine[...]
    for other in got:
        total = total + other[...].astype(F32)
    total = total * gain[pl.ds(pl.multiple_of(core * half, LANES), half), :].astype(F32)
    piece[...] = total
    squares[...] = jnp.full(squares.shape, jnp.sum(total * total), F32)


def scale_kernel(count, own, got_y, got_c, got_cy, s0, s1, s2, s3, out):
    _, y, core = place()
    half, wide = own.shape
    squares = ((s0[...] + s1[...]) + (s2[...] + s3[...]))[:1, :1]
    factor = 1.0 / jnp.maximum(1.0, jnp.sqrt(squares / count))
    for dc, dy, piece in ((0, 0, own), (0, 1, got_y), (1, 0, got_c), (1, 1, got_cy)):
        at = pl.ds(pl.multiple_of((core ^ dc) * half, LANES), half)
        out[at, pl.ds(pl.multiple_of((y ^ dy) * wide, LANES), wide)] = piece[...] * factor


def blocks(rows, order, acts, cot, own, other):
    shard, _, core = place()
    half = rows // 2
    for side, (ref, c) in enumerate(((own, core), (other, 1 - core))):
        for j in range(0, len(order), 2):
            pair = jnp.concatenate([ref[j, :half, :], ref[j + 1, :half, :]], axis=0)
            product = ab(cot[...], pair, 1, 1)
            for k in (j, j + 1):
                col = pl.ds(pl.multiple_of((shard ^ order[k]) * rows + c * half, LANES), half)
                gains = ref[k, half : half + 2, :half].astype(F32)
                gain = jnp.where(c == 0, gains[:1], gains[1:2])
                h = product[:, (k - j) * half : (k - j + 1) * half] * gain
                yield side * len(order) + k, col, h, h * acts[:, col].astype(F32)


def near_kernel(rows, order, acts, cot, own, other, held, inner, rstd):
    half, total = rows // 2, jnp.zeros(inner.shape, F32)
    for n, _, h, product in blocks(rows, order, acts, cot, own, other):
        held[:, n * half : (n + 1) * half] = h
        total = total + product
    inner[...] = total
    rstd[...] = jnp.broadcast_to(row_rstd(acts[...].astype(F32)), rstd.shape)


def far_kernel(rows, order, order_near, acts, cot, own, other, held, inner, rstd, out, scaled):
    shard, _, core = place()
    half, width = rows // 2, acts.shape[1]
    total = inner[...]
    for n, _, h, product in blocks(rows, order, acts, cot, own, other):
        scaled[:, n * half : (n + 1) * half] = h
        total = total + product
    mean = jnp.sum(total, axis=-1, keepdims=True) * (1.0 / width)
    scale = rstd[:, :1]
    back = scale * scale * scale * mean
    for source, shards in ((held, order_near), (scaled, order)):
        for side in range(2):
            for k, j in enumerate(shards):
                n = side * len(shards) + k
                col = pl.ds(pl.multiple_of((shard ^ j) * rows + (core ^ side) * half, LANES), half)
                h = source[:, n * half : (n + 1) * half]
                out[:, col] = (scale * h - acts[:, col].astype(F32) * back).astype(out.dtype)


def call(kernel, shapes, *args, scratch=(), space=VMEM):
    return pl.pallas_call(
        kernel,
        out_shape=shapes,
        in_specs=[space] * len(args),
        out_specs=jax.tree.map(lambda _: VMEM, shapes),
        scratch_shapes=scratch,
        compiler_params=pltpu.CompilerParams(vmem_limit_bytes=48 * 2**20),
    )(*args)


def fast(shards, reps, activations, value_grad, norm_gain, value_weight):
    batches, tokens, width = activations.shape
    rows, columns = value_weight.shape
    zs, half, wide = shards // 2, rows // 2, columns // 2
    tokens *= batches
    acts, cot = activations.reshape(tokens, width), value_grad.reshape(tokens, columns)

    def swap(value, over_shard, over_rep):
        pairs = [
            (s * reps + r, (s ^ over_shard) * reps + (r ^ over_rep)) for s in range(shards) for r in range(reps)
        ]
        return lax.ppermute(value, ("shard", "rep"), pairs)

    def like(*shape, kind=F32):
        return jax.ShapeDtypeStruct(shape, kind)

    acts_other, cot_other = swap(acts, 0, 1), swap(cot, 0, 1)

    core = lax.axis_index("rep") % 2
    gains = jnp.pad(norm_gain.reshape(2, half), ((0, 6), (0, columns - half)))
    held = jnp.concatenate([lax.dynamic_slice_in_dim(value_weight, core * half, half, 0), gains], axis=0)
    near = [2 * k for k in range(zs)]
    held = jnp.stack([held] + [swap(held, 2 * k, 0) for k in range(1, zs)])
    held_other = swap(held, 0, 1)
    held_far = swap(held, 1, 0)
    far_other = swap(held_far, 0, 1)

    scratch = [pltpu.VMEM((tokens, columns), BF16)] * 2 + [pltpu.VMEM((tokens, 2 * zs * half), BF16)]
    part = call(
        functools.partial(own_kernel, zs, rows),
        like(4, zs * half, wide),
        pltpu.with_memory_space_constraint(acts, pltpu.HBM), pltpu.with_memory_space_constraint(cot, pltpu.HBM),
        scratch=[pltpu.VMEM(acts.shape, BF16), pltpu.VMEM(cot.shape, BF16)] + scratch + [pltpu.SemaphoreType.DMA((2,))],
        space=pl.BlockSpec(memory_space=pltpu.HBM),
    )
    send_d, send_y, send_x, keep = call(
        functools.partial(grad_kernel, zs, rows),
        (like(zs * half, wide, kind=BF16),) * 3 + (like(zs * half, wide),),
        acts_other, cot_other, part,
        scratch=scratch,
    )
    got_d, got_y, got_x = swap(send_d, 1, 2), swap(send_y, 0, 2), swap(send_x, 1, 0)
    mine, *sends = call(
        functools.partial(plane_kernel, zs),
        (like(half, wide),) + (like(half, wide, kind=BF16),) * (zs - 1),
        keep, got_x, got_y, got_d,
    )
    got = [swap(sends[k - 1], 2 * k, 0) for k in range(1, zs)]
    own, squares = call(
        line_kernel,
        (like(half, wide), like(8, LANES)),
        mine, *got, norm_gain[:, None],
    )
    got_y = swap(own, 0, 2)
    got_c = swap(own, 0, 1)
    got_cy = swap(got_y, 0, 1)
    squares = squares + swap(squares, 0, 1)
    others = [swap(squares, 2 * k, 0) for k in range(1, zs)]
    squares = (squares + others[0]) + (others[1] + others[2])
    parts = [squares, swap(squares, 1, 0), swap(squares, 0, 2), swap(squares, 1, 2)]
    update = call(
        functools.partial(scale_kernel, float(width * columns)),
        like(rows, columns),
        own, got_y, got_c, got_cy, *parts,
    )
    h, inner, rstd = call(
        functools.partial(near_kernel, rows, near),
        (like(tokens, width // 2), like(tokens, half), like(tokens, LANES)),
        acts, cot, held, held_other,
    )
    result = call(
        functools.partial(far_kernel, rows, [j ^ 1 for j in near], near),
        like(tokens, width, kind=BF16),
        acts, cot, held_far, far_other, h, inner, rstd,
        scratch=[pltpu.VMEM((tokens, width // 2), F32)],
    )
    return result.reshape(activations.shape), update


def plain(shards, reps, activations, value_grad, norm_gain, value_weight):
    gain_all, weight_all = (
        lax.all_gather(norm_gain, "shard", axis=0, tiled=True),
        lax.all_gather(value_weight, "shard", axis=0, tiled=True),
    )
    gain = gain_all.astype(F32)
    width = activations.shape[2]
    columns = value_grad.shape[2]

    def one_batch(total, inputs):
        block, cotangent = inputs
        values = block.astype(F32)
        rstd = row_rstd(values)
        normed = (values * rstd * gain).astype(BF16)
        total = total + ab(normed, cotangent, 0, 0)
        scaled = jnp.dot(cotangent, weight_all.T, preferred_element_type=F32) * gain
        inner = jnp.mean(scaled * values, axis=-1, keepdims=True)
        result = (rstd * scaled - values * rstd * rstd * rstd * inner).astype(BF16)
        return (total, result)

    start = jnp.zeros((width, columns), F32)
    grad_full, input_grad = lax.scan(one_batch, start, (activations, value_grad))
    partial_rows = lax.psum_scatter(grad_full, "shard", scatter_dimension=0, tiled=True)
    summed = lax.psum(partial_rows, "rep")
    squares = lax.psum(jnp.sum(summed * summed), "shard")
    factor = 1.0 / jnp.maximum(1.0, jnp.sqrt(squares / (width * columns)))
    return (input_grad, summed * factor)


def solution(mesh):
    shards, reps = mesh.shape["shard"], mesh.shape["rep"]

    def on_device(activations, value_grad, norm_gain, value_weight):
        rows, columns = value_weight.shape
        fits = (shards, reps) == (8, 4) and rows % 256 == 0 and columns % 256 == 0 and rows <= columns
        return (fast if fits else plain)(shards, reps, activations, value_grad, norm_gain, value_weight)

    in_specs = (
        P(None, ("shard", "rep"), None),
        P(None, ("shard", "rep"), None),
        P("shard"),
        P("shard", None),
    )
    out_specs = (P(None, ("shard", "rep"), None), P("shard", None))
    return jax.shard_map(on_device, mesh=mesh, in_specs=in_specs, out_specs=out_specs, check_vma=False)
```
